32 devices in a mesh: dp: 16 (over z, x, core), mp: 2 (over y).
Axes of the slice: x: 2, y: 2, z: 4, core: 2. Of those that a mesh axis runs over, the one named last changes fastest.
Arguments:
- inputs_store: bfloat16 [512, 128], replicated, may hold values from -6 to 6
- window: int32 [16], replicated, may hold values from 0 to 511
- targets_store: bfloat16 [512, 4096], P(None, ('dp', 'mp')), may hold values from -6 to 6
- jac_store: bfloat16 [512, 4096, 128], P(None, ('dp', 'mp')), may hold values from -4 to 4
- first_weight: bfloat16 [128, 1024], replicated, may hold values from -0.5 to 0.5
- first_bias: bfloat16 [1024], replicated, may hold values from -3 to 3
- hidden_weight: bfloat16 [1024, 1024], P(None, 'mp'), may hold values from -0.1875 to 0.1875
- hidden_bias: bfloat16 [1024], P('mp'), may hold values from -3 to 3
- decoder_weight: bfloat16 [4096, 1024], P(('dp', 'mp')), may hold values from -0.1875 to 0.1875
Outputs:
- first_weights: float32 [128, 1024], replicated
- first_biases: float32 [1024], replicated
- hidden_weights: float32 [1024, 1024], P(None, 'mp')
- hidden_biases: float32 [1024], P('mp')
- decoder_grad: float32 [4096, 1024], P(('dp', 'mp'))
The draws below stay inside these ranges and needn't reach their ends.
Inputs may be any that keep to these rules, and one draw needn't show every extreme that they name: `window`: indices of stored samples; an index may repeat.
All inputs are finite; a program needn't handle non-finite values.
Results may differ from the reference program's by a relative error of at most 0.011.
Values may be sent and summed in bfloat16 or wider, within the bound.
A program may use at most 64 MiB of HBM per device.

```python
import math
import jax
import jax.numpy as jnp
from jax import lax

RANK = 128
H = 1024
OUT = 4096
NSTORE = 512
SAMPLES = 16
N_DP = 16
N_MP = 2


def place_ends(values, stream_key, low, high):
    dims = values.shape
    place = [jax.random.randint(jax.random.fold_in(stream_key, axis), (), 0, dims[axis]) for axis in range(len(dims))]
    values = values.at[tuple(place)].set(low)
    longest = dims.index(max(dims))
    place[longest] = (place[longest] + 1) % dims[longest]
    return values.at[tuple(place)].set(high)


def steps_of(key, shape, pieces, low, top_value):
    loudness = 1.0
    for axis_at, blocks in pieces:
        steps = jax.random.uniform(jax.random.fold_in(jax.random.fold_in(key, 6), axis_at), (blocks,), jnp.float32, low / len(pieces), top_value / len(pieces))
        loudness = loudness * jnp.repeat(jnp.exp(steps), shape[axis_at] // blocks).reshape((-1,) + (1,) * (len(shape) - 1 - axis_at))
    return loudness


def centred(key, extent, scale, most, pieces=(), kind=jnp.bfloat16):
    factor_of = steps_of(key, extent, pieces, -0.22, 0.18) if pieces else 1.0
    values = jax.random.normal(key, extent, jnp.float32) * scale * factor_of
    return jnp.minimum(jnp.maximum(values, -most), most).astype(kind)


def setup_inputs(seed: int = 0) -> dict:
    keys = jax.random.split(jax.random.key(seed), 10)
    return {
        "inputs_store": centred(keys[0], (NSTORE, RANK), 1.0, 6.0),
        "window": place_ends(jax.random.randint(keys[1], (SAMPLES,), 0, NSTORE), jax.random.fold_in(keys[1], 1), 0, NSTORE - 1).astype(jnp.int32),
        "targets_store": centred(keys[2], (NSTORE, OUT), 1.0, 6.0, ((1, 32),)),
        "jac_store": centred(keys[3], (NSTORE, OUT, RANK), 0.3, 4.0, ((1, 32),)),
        "first_weight": centred(keys[4], (RANK, H), RANK ** -0.5, 0.5),
        "first_bias": centred(keys[5], (H,), 0.5, 3.0),
        "hidden_weight": centred(keys[6], (H, H), H ** -0.5, 0.1875, ((1, 2),)),
        "hidden_bias": centred(keys[7], (H,), 0.5, 3.0, ((0, 2),)),
        "decoder_weight": centred(keys[8], (OUT, H), H ** -0.5, 0.1875, ((0, 32),)),
    }


def rounded(values):
    return lax.optimization_barrier(values.astype(jnp.bfloat16)).astype(jnp.float32)


def reference(inputs_store, window, targets_store, jac_store, first_weight, first_bias, hidden_weight, hidden_bias, decoder_weight):
    block = math.gcd(SAMPLES, 8)
    out_rows = OUT // (N_DP * N_MP)
    weight_one = first_weight.astype(jnp.float32)
    weight_two = hidden_weight.astype(jnp.float32)
    readout_weight = decoder_weight.astype(jnp.float32)
    dec_groups = readout_weight.reshape(N_DP, N_MP, out_rows, H)

    def block_step(totals, indices):
        grad_one, bias_one, grad_two, bias_two, decoder_gradient = totals
        inputs = inputs_store[indices]
        targets = targets_store[indices].astype(jnp.float32)
        jacobians = jac_store[indices].astype(jnp.float32)
        first_pre = jnp.dot(inputs, first_weight, preferred_element_type=jnp.float32) + first_bias.astype(jnp.float32)
        first_act = jnp.tanh(first_pre)
        first_slope = 1.0 - first_act * first_act
        first_tan = rounded(first_slope[:, None, :] * weight_one[None])
        first_round = rounded(first_act)
        hidden_lin = jnp.einsum("srh,hk->srk", first_tan, weight_two)
        hidden_pre = jnp.einsum("sh,hk->sk", first_round, weight_two) + hidden_bias.astype(jnp.float32)
        hidden_act = jnp.tanh(hidden_pre)
        hidden_slope = 1.0 - hidden_act * hidden_act
        hidden_tangent = rounded(hidden_slope[:, None, :] * hidden_lin)
        hidden_rounded_state = rounded(hidden_act)
        outputs_net = jnp.einsum("sk,ok->so", hidden_rounded_state, readout_weight)
        jacobian_predicted = jnp.einsum("mvn,an->mav", hidden_tangent, readout_weight)
        output_residual = rounded(outputs_net - targets)
        jacobian_residual = rounded(jacobian_predicted - jacobians)
        decoder_gradient = decoder_gradient + jnp.einsum("qi,qm->im", output_residual, hidden_rounded_state) + jnp.einsum("hzy,hym->zm", jacobian_residual, hidden_tangent)
        miss_groups = output_residual.reshape(block, N_DP, N_MP, out_rows)
        jac_groups = jacobian_residual.reshape(block, N_DP, N_MP, out_rows, RANK)
        act_back = jnp.sum(rounded(jnp.einsum("sdmk,dmkh->smh", miss_groups, dec_groups)), axis=1)
        tan_back = jnp.sum(rounded(jnp.einsum("sdmkr,dmkh->smrh", jac_groups, dec_groups)), axis=1)
        lin_back = tan_back * hidden_slope[:, None, :]
        pre_back = act_back * hidden_slope - 2.0 * hidden_act * hidden_slope * jnp.sum(tan_back * hidden_lin, axis=1)
        lin_round = rounded(lin_back)
        pre_round = rounded(pre_back)
        grad_two = grad_two + jnp.einsum("sh,sk->hk", first_round, pre_round) + jnp.einsum("srh,srk->hk", first_tan, lin_round)
        bias_two = bias_two + jnp.sum(pre_back, axis=0)
        tan_lower = jnp.einsum("srk,hk->srh", lin_round, weight_two)
        act_lower = jnp.einsum("sk,hk->sh", pre_round, weight_two)
        pre_lower = act_lower * first_slope - 2.0 * first_act * first_slope * jnp.sum(tan_lower * weight_one[None], axis=1)
        grad_one = grad_one + jnp.einsum("sr,sh->rh", inputs.astype(jnp.float32), pre_lower, precision=lax.Precision.HIGHEST) + jnp.sum(tan_lower * first_slope[:, None, :], axis=0)
        bias_one = bias_one + jnp.sum(pre_lower, axis=0)
        return (grad_one, bias_one, grad_two, bias_two, decoder_gradient), None

    start_totals = (jnp.zeros((RANK, H), jnp.float32), jnp.zeros((H,), jnp.float32), jnp.zeros((H, H), jnp.float32), jnp.zeros((H,), jnp.float32), jnp.zeros((OUT, H), jnp.float32))
    totals, unused = lax.scan(block_step, start_totals, window.reshape(-1, block))
    return totals[0], totals[1], totals[2], totals[3], totals[4]
```

```python
import jax
import jax.numpy as jnp
from jax import lax
from jax.sharding import PartitionSpec as P

F32 = jnp.float32
BF16 = jnp.bfloat16


def dot(spec, a, b):
    return jnp.einsum(spec, a, b, preferred_element_type=F32)


def on_device(
    inputs_store,
    window,
    targets_store,
    jac_store,
    first_weight,
    first_bias,
    hidden_weight,
    hidden_bias,
    decoder_weight,
):
    dp, mp = lax.axis_size("dp"), lax.axis_size("mp")
    at = lax.axis_index("dp")
    samples = window.shape[0]
    each = samples // dp
    rank, hidden = first_weight.shape
    own_hidden = hidden_weight.shape[1]
    out_rows = decoder_weight.shape[0]

    share = hidden // dp
    pad = 16
    piece = jnp.concatenate(
        [
            lax.dynamic_slice_in_dim(hidden_weight, at * share, share),
            jnp.broadcast_to(hidden_bias[None], (pad, own_hidden)),
        ],
        axis=0,
    )
    pieces = lax.all_gather(piece, ("dp", "mp"), axis=0).reshape(dp, mp, share + pad, own_hidden)
    weight_two = pieces[:, :, :share].transpose(0, 2, 1, 3).reshape(hidden, mp * own_hidden)
    bias_two = pieces[0, :, share].reshape(mp * own_hidden).astype(F32)

    decoder_group = lax.all_gather(decoder_weight, "dp", axis=0)

    inputs = inputs_store[window]
    weight_one = first_weight.astype(F32)
    first_act = jnp.tanh(dot("sr,rh->sh", inputs, first_weight) + first_bias.astype(F32))
    first_slope = 1.0 - first_act * first_act
    first_tan = (first_slope[:, None, :] * weight_one[None]).astype(BF16)
    first_round = first_act.astype(BF16)

    hidden_act = jnp.tanh(dot("sh,hk->sk", first_round, weight_two) + bias_two)
    hidden_slope = 1.0 - hidden_act * hidden_act
    hidden_tan = (hidden_slope[:, None, :] * dot("srh,hk->srk", first_tan, weight_two)).astype(BF16)
    hidden_round = hidden_act.astype(BF16)

    targets = targets_store[window].astype(F32)
    jacobians = jac_store[window].astype(F32)
    out_miss = (dot("sk,ok->so", hidden_round, decoder_weight) - targets).astype(BF16)
    jac_miss = (dot("srk,ok->sor", hidden_tan, decoder_weight) - jacobians).astype(BF16)

    extra = -(-out_rows // rank)
    rider = jnp.pad(out_miss, ((0, 0), (0, extra * rank - out_rows))).reshape(samples, extra, rank)
    packed = jnp.concatenate([jac_miss, rider], axis=1).reshape(dp, each, out_rows + extra, rank)
    mine = lax.all_to_all(packed, "dp", split_axis=0, concat_axis=0, tiled=True)

    decoder_grad = dot("so,sk->ok", out_miss, hidden_round) + dot(
        "sor,srk->ok", jac_miss, hidden_tan
    )

    out_mine = mine[:, :, out_rows:].reshape(dp, each, extra * rank)[:, :, :out_rows]
    tan_part = dot("pcor,pok->crk", mine[:, :, :out_rows], decoder_group).astype(BF16)
    act_part = dot("pco,pok->ck", out_mine, decoder_group).astype(BF16)
    part = jnp.concatenate([tan_part, act_part[:, None]], axis=1)
    part = part.reshape(each, rank + 1, mp, own_hidden).transpose(2, 0, 1, 3)
    back = jnp.sum(
        lax.all_to_all(part, "mp", split_axis=0, concat_axis=0, tiled=True).astype(F32), axis=0
    )
    tan_back, act_back = back[:, :rank], back[:, rank]

    tan_own = lax.dynamic_slice_in_dim(first_tan, at * each, each)
    round_own = lax.dynamic_slice_in_dim(first_round, at * each, each)
    lin_own = dot("srh,hk->srk", tan_own, hidden_weight)
    act_own = jnp.tanh(dot("sh,hk->sk", round_own, hidden_weight) + hidden_bias.astype(F32))
    slope_own = 1.0 - act_own * act_own
    lin_back = tan_back * slope_own[:, None, :]
    pre_back = act_back * slope_own - 2.0 * act_own * slope_own * jnp.sum(tan_back * lin_own, axis=1)
    send = jnp.concatenate([lin_back, pre_back[:, None]], axis=1).astype(BF16)

    full = lax.all_gather(send, "dp", axis=0, tiled=True)
    lin_round, pre_round = full[:, :rank], full[:, rank]
    hidden_weights = dot("sh,sk->hk", first_round, pre_round) + dot(
        "srh,srk->hk", first_tan, lin_round
    )
    hidden_biases = jnp.sum(pre_round.astype(F32), axis=0)
    tan_lower = dot("srk,hk->srh", lin_round, hidden_weight)
    act_lower = dot("sk,hk->sh", pre_round, hidden_weight)
    pre_lower = act_lower * first_slope - 2.0 * first_act * first_slope * jnp.sum(
        tan_lower * weight_one[None], axis=1
    )
    weight_part = jnp.einsum(
        "sr,sh->rh", inputs.astype(F32), pre_lower, precision=lax.Precision.HIGHEST
    ) + jnp.sum(tan_lower * first_slope[:, None, :], axis=0)
    bias_part = jnp.sum(pre_lower, axis=0)
    both = jnp.concatenate([weight_part, bias_part[None]], axis=0).astype(BF16)
    total = jnp.sum(lax.all_gather(both, "mp", axis=0).astype(F32), axis=0)
    return total[:rank], total[rank], hidden_weights, hidden_biases, decoder_grad


def solution(mesh):
    placed = (
        P(),
        P(),
        P(None, ("dp", "mp")),
        P(None, ("dp", "mp"), None),
        P(),
        P(),
        P(None, "mp"),
        P("mp"),
        P(("dp", "mp"), None),
    )
    return jax.shard_map(
        on_device,
        mesh=mesh,
        in_specs=placed,
        out_specs=(P(), P(), P(None, "mp"), P("mp"), P(("dp", "mp"), None)),
        check_vma=False,
    )
```

```python
import jax
import jax.numpy as jnp
from jax import lax
from jax.sharding import PartitionSpec as P

F32 = jnp.float32
BF16 = jnp.bfloat16


def dot(spec, a, b):
    return jnp.einsum(spec, a, b, preferred_element_type=F32)


def on_device(
    inputs_store,
    window,
    targets_store,
    jac_store,
    first_weight,
    first_bias,
    hidden_weight,
    hidden_bias,
    decoder_weight,
):
    dp, mp = lax.axis_size("dp"), lax.axis_size("mp")
    at = lax.axis_index("dp")
    samples = window.shape[0]
    each = samples // dp
    rank, hidden = first_weight.shape
    own_hidden = hidden_weight.shape[1]
    out_rows = decoder_weight.shape[0]

    me = lax.axis_index("mp")
    parity = at % 2
    half = hidden // 2
    swap = [(i, i ^ 1) for i in range(dp)]
    my_half = lax.dynamic_slice_in_dim(hidden_weight, parity * half, half)
    weights, biases = [hidden_weight], [hidden_bias]
    for shift in range(1, mp):
        turn = [(i, (i + shift) % mp) for i in range(mp)]
        biases.append(lax.ppermute(hidden_bias, "mp", turn))
        got = lax.ppermute(my_half, "mp", turn)
        other = lax.ppermute(got, "dp", swap)
        weights.append(
            jnp.concatenate(
                [jnp.where(parity == 0, got, other), jnp.where(parity == 0, other, got)], axis=0
            )
        )

    def in_order(blocks, axis):
        if mp == 2:
            own, peer = blocks
            picked = [jnp.where(me == 0, own, peer), jnp.where(me == 0, peer, own)]
        else:
            stacked = jnp.stack(blocks)
            picked = [
                lax.dynamic_index_in_dim(stacked, (me - j + mp) % mp, 0, keepdims=False)
                for j in range(mp)
            ]
        return jnp.concatenate(picked, axis=axis)

    weight_two = in_order(weights, 1)
    bias_two = in_order(biases, 0).astype(F32)

    decoder_group = lax.all_gather(decoder_weight, "dp", axis=0)

    inputs = inputs_store[window]
    weight_one = first_weight.astype(F32)
    first_act = jnp.tanh(dot("sr,rh->sh", inputs, first_weight) + first_bias.astype(F32))
    first_slope = 1.0 - first_act * first_act
    first_tan = (first_slope[:, None, :] * weight_one[None]).astype(BF16)
    first_round = first_act.astype(BF16)

    hidden_act = jnp.tanh(dot("sh,hk->sk", first_round, weight_two) + bias_two)
    hidden_slope = 1.0 - hidden_act * hidden_act
    hidden_tan = (hidden_slope[:, None, :] * dot("srh,hk->srk", first_tan, weight_two)).astype(BF16)
    hidden_round = hidden_act.astype(BF16)

    targets = targets_store[window].astype(F32)
    jacobians = jac_store[window].astype(F32)
    out_miss = (dot("sk,ok->so", hidden_round, decoder_weight) - targets).astype(BF16)
    jac_miss = (dot("srk,ok->sor", hidden_tan, decoder_weight) - jacobians).astype(BF16)

    extra = -(-out_rows // rank)
    rider = jnp.pad(out_miss, ((0, 0), (0, extra * rank - out_rows))).reshape(samples, extra, rank)
    packed = jnp.concatenate([jac_miss, rider], axis=1).reshape(dp, each, out_rows + extra, rank)
    mine = lax.all_to_all(packed, "dp", split_axis=0, concat_axis=0, tiled=True)

    decoder_grad = dot("so,sk->ok", out_miss, hidden_round) + dot(
        "sor,srk->ok", jac_miss, hidden_tan
    )

    out_mine = mine[:, :, out_rows:].reshape(dp, each, extra * rank)[:, :, :out_rows]
    tan_part = dot("pcor,pok->crk", mine[:, :, :out_rows], decoder_group).astype(BF16)
    act_part = dot("pco,pok->ck", out_mine, decoder_group).astype(BF16)
    part = jnp.concatenate([tan_part, act_part[:, None]], axis=1)
    part = part.reshape(each, rank + 1, mp, own_hidden).transpose(2, 0, 1, 3)
    back = jnp.sum(
        lax.all_to_all(part, "mp", split_axis=0, concat_axis=0, tiled=True).astype(F32), axis=0
    )
    tan_back, act_back = back[:, :rank], back[:, rank]

    tan_own = lax.dynamic_slice_in_dim(first_tan, at * each, each)
    round_own = lax.dynamic_slice_in_dim(first_round, at * each, each)
    lin_own = dot("srh,hk->srk", tan_own, hidden_weight)
    act_own = jnp.tanh(dot("sh,hk->sk", round_own, hidden_weight) + hidden_bias.astype(F32))
    slope_own = 1.0 - act_own * act_own
    lin_back = tan_back * slope_own[:, None, :]
    pre_back = act_back * slope_own - 2.0 * act_own * slope_own * jnp.sum(tan_back * lin_own, axis=1)
    send = jnp.concatenate([lin_back, pre_back[:, None]], axis=1).astype(BF16)

    full = lax.all_gather(send, "dp", axis=0, tiled=True)
    lin_round, pre_round = full[:, :rank], full[:, rank]
    hidden_weights = dot("sh,sk->hk", first_round, pre_round) + dot(
        "srh,srk->hk", first_tan, lin_round
    )
    hidden_biases = jnp.sum(pre_round.astype(F32), axis=0)
    tan_lower = dot("srk,hk->srh", lin_round, hidden_weight)
    act_lower = dot("sk,hk->sh", pre_round, hidden_weight)
    pre_lower = act_lower * first_slope - 2.0 * first_act * first_slope * jnp.sum(
        tan_lower * weight_one[None], axis=1
    )
    weight_part = jnp.einsum(
        "sr,sh->rh", inputs.astype(F32), pre_lower, precision=lax.Precision.HIGHEST
    ) + jnp.sum(tan_lower * first_slope[:, None, :], axis=0)
    bias_part = jnp.sum(pre_lower, axis=0)
    both = jnp.concatenate([weight_part, bias_part[None]], axis=0).astype(BF16)
    total = jnp.sum(lax.all_gather(both, "mp", axis=0).astype(F32), axis=0)
    return total[:rank], total[rank], hidden_weights, hidden_biases, decoder_grad


def solution(mesh):
    placed = (
        P(),
        P(),
        P(None, ("dp", "mp")),
        P(None, ("dp", "mp"), None),
        P(),
        P(),
        P(None, "mp"),
        P("mp"),
        P(("dp", "mp"), None),
    )
    return jax.shard_map(
        on_device,
        mesh=mesh,
        in_specs=placed,
        out_specs=(P(), P(), P(None, "mp"), P("mp"), P(("dp", "mp"), None)),
        check_vma=False,
    )
```
